32 devices in a mesh: cuts: 8 (over y, x, core), mode: 4 (over z).
Axes of the slice: x: 2, y: 2, z: 4, core: 2. Of those that a mesh axis runs over, the one named last changes fastest.
Arguments:
- stem: float32 [8, 16, 16, 32768], P('cuts', 'mode'), may hold values from -1.5 to 1.5
- left: float32 [6, 2, 512, 512], P(None, None, 'mode'), may hold values from -0.25 to 0.25
- right: float32 [512, 512], replicated, may hold values from -0.25 to 0.25
- slice_bits: int32 [8, 6], P('cuts'), may hold values from 0 to 1
- leg_order: int32 [6, 9], replicated, may hold values from 0 to 8, each once within a row
Outputs:
- amplitudes: float32 [16, 16, 32768], P(None, 'mode', 'cuts')
The draws below stay inside these ranges and needn't reach their ends.
Inputs may be any that keep to these rules, and one draw needn't show every extreme that they name: slice_bits[s, t] is the value of branch t's cut bond in slice s. Each row of leg_order is a permutation of 0 to 8.
All inputs are finite; a program needn't handle non-finite values.
Results may differ from the reference program's by a relative error of at most 0.00018.
Values sent between devices are 32-bit elements; how exact they have to be, the bound alone decides.
No kernel may reach another device: no remote copies, remote signals or barrier semaphores. Data moves between devices by JAX's collectives and lax.ppermute only.
A program may use at most 128 MiB of HBM per device.

```python
import jax
import jax.numpy as jnp
from jax import lax

LEGS = 9
BRANCH = 512
TAIL_MODES = 15
TAIL = 32768
HEAD = 16
BRANCHES = 6
SLICES = 8


def touch_ends(values, rng, low, largest):
    shape = values.shape
    place = [jax.random.randint(jax.random.fold_in(rng, axis), (), 0, shape[axis]) for axis in range(len(shape))]
    values = values.at[tuple(place)].set(low)
    longest = shape.index(max(shape))
    place[longest] = (place[longest] + 1) % shape[longest]
    return values.at[tuple(place)].set(largest)


def shard_levels(own_key, extent, pieces, least, largest):
    def one(axis_at, parts):
        steps = jax.random.uniform(jax.random.fold_in(jax.random.fold_in(own_key, 6), axis_at), (parts,), jnp.float32, least / len(pieces), largest / len(pieces))
        return jnp.repeat(jnp.exp(steps), extent[axis_at] // parts).reshape((-1,) + (1,) * (len(extent) - axis_at - 1))

    level = one(*pieces[0])
    for cut in pieces[1:]:
        level = level * one(*cut)
    return level


def scatter_about(rng, shape, scale, limit, shards=(), held_as=jnp.bfloat16):
    factor_of = shard_levels(rng, shape, shards, -0.22, 0.18) if shards else 1.0
    values = jax.random.normal(rng, shape, jnp.float32) * scale * factor_of
    return jnp.minimum(jnp.maximum(values, -limit), limit).astype(held_as)


def setup_inputs(seed: int = 0) -> dict:
    streams_of = jax.random.split(jax.random.key(seed), 6)
    return {
        "stem": scatter_about(streams_of[0], (SLICES, HEAD, HEAD, TAIL), 0.25, 1.5, ((0, 8), (1, 4)), jnp.float32),
        "left": scatter_about(streams_of[1], (BRANCHES, 2, BRANCH, BRANCH), BRANCH ** -0.5, 0.25, ((2, 4),), jnp.float32),
        "right": scatter_about(streams_of[2], (BRANCH, BRANCH), BRANCH ** -0.5, 0.25, (), jnp.float32),
        "slice_bits": touch_ends(jax.random.randint(streams_of[3], (SLICES, BRANCHES), 0, 2), jax.random.fold_in(streams_of[3], 1), 0, 1).astype(jnp.int32),
        "leg_order": jax.vmap(lambda own: jax.random.permutation(own, LEGS))(jax.random.split(streams_of[4], BRANCHES)).reshape((BRANCHES, LEGS)).astype(jnp.int32),
    }


HIGHEST_PRECISION = lax.Precision.HIGHEST


def leg_columns(leg_map, leg_count):
    indices = jnp.arange(2 ** leg_count, dtype=jnp.int32)
    shifts = (leg_count - 1 - leg_map).astype(jnp.int32)
    chosen = jnp.right_shift(indices[:, None], shifts[None, :]) & 1
    powers = jnp.left_shift(jnp.ones((leg_count,), jnp.int32), (leg_count - 1 - jnp.arange(leg_count, dtype=jnp.int32)))
    return jnp.sum(chosen * powers[None, :], axis=1).astype(jnp.int32)


def run_absorb(tensor, matrix, first, leg_count):
    branch_size = 2 ** leg_count
    after = tensor.size // (2 ** first * branch_size)
    shaped = tensor.reshape(2 ** first, branch_size, after)
    result = jnp.einsum("ji,pir->pjr", matrix, shaped, precision=HIGHEST_PRECISION)
    return result.reshape(tensor.shape)


def head_absorb(tensor, matrix, leg_count):
    inner = 2 ** (leg_count - 4)
    shaped = tensor.reshape(16, 16, inner, -1)
    blocks = matrix.reshape(16, inner, 16, inner)
    result = jnp.einsum("abcd,cxdr->axbr", blocks, shaped, precision=HIGHEST_PRECISION)
    return result.reshape(tensor.shape)


def pair_absorb(tensor, matrix, leg_count):
    inner = 2 ** (leg_count - 2)
    shaped = tensor.reshape(4, 4, 16, inner, -1)
    blocks = matrix.reshape(4, inner, 4, inner)
    result = jnp.einsum("bdce,acxer->abxdr", blocks, shaped, precision=HIGHEST_PRECISION)
    return result.reshape(tensor.shape)


def reference(stem, left, right, slice_bits, leg_order):
    total_modes = 8 + TAIL_MODES
    permuted = [jnp.take(right, leg_columns(leg_order[branch], LEGS), axis=1) for branch in range(6)]

    def one_slice(summed, inputs):
        tensor, bits = inputs
        matrices = [jnp.dot(left[branch][bits[branch]], permuted[branch], precision=HIGHEST_PRECISION) for branch in range(6)]
        tensor = run_absorb(tensor, matrices[0], total_modes - LEGS, LEGS)
        tensor = run_absorb(tensor, matrices[1], 6, LEGS)
        tensor = run_absorb(tensor, matrices[2], 4, LEGS)
        tensor = head_absorb(tensor, matrices[3], LEGS)
        tensor = run_absorb(tensor, matrices[4], total_modes - LEGS, LEGS)
        tensor = pair_absorb(tensor, matrices[5], LEGS)
        return summed + tensor, None

    summed, unused = lax.scan(one_slice, jnp.zeros(stem.shape[1:], stem.dtype), (stem, slice_bits))
    return summed
```

```python
import functools

import jax
import jax.numpy as jnp
from jax import lax
from jax.experimental import pallas as pl
from jax.experimental.pallas import tpu as pltpu
from jax.sharding import PartitionSpec as P


BF16 = jnp.bfloat16
F32 = jnp.float32
VMEM_LIMIT = 60 * 1024 * 1024


def leg_columns(leg_map, leg_count, indices):
    shifts = leg_count - 1 - leg_map
    chosen = jnp.right_shift(indices[:, None], shifts[None, :]) & 1
    powers = jnp.left_shift(
        jnp.ones((leg_count,), jnp.int32), leg_count - 1 - jnp.arange(leg_count, dtype=jnp.int32)
    )
    return jnp.sum(chosen * powers[None, :], axis=1)


def halves(value):
    high = value.astype(BF16)
    return high, (value - high.astype(F32)).astype(BF16)


def dot(a, b, contract=((1,), (0,))):
    return lax.dot_general(a, b, (contract, ((), ())), preferred_element_type=F32)


def product(a, b, contract=((1,), (0,))):
    return dot(a[0], b[0], contract) + (dot(a[0], b[1], contract) + dot(a[1], b[0], contract))


def order_kernel(columns_ref, right_ref, high_ref, low_ref):
    size = right_ref.shape[0]
    picks = lax.broadcasted_iota(jnp.int32, (size, size), 0) == columns_ref[0]
    chosen = jnp.where(picks, 1.0, 0.0).astype(BF16)
    high, low = halves(right_ref[...])
    high_ref[0] = dot(high, chosen).astype(BF16)
    low_ref[0] = dot(low, chosen).astype(BF16)


def order(right, columns):
    count, _, size = columns.shape
    block = pl.BlockSpec((1, size, size), lambda t: (t, 0, 0))
    return pl.pallas_call(
        order_kernel,
        grid=(count,),
        in_specs=[
            pl.BlockSpec((1, 1, size), lambda t: (t, 0, 0)),
            pl.BlockSpec((size, size), lambda t: (0, 0)),
        ],
        out_specs=[block] * 2,
        out_shape=[jax.ShapeDtypeStruct((count, size, size), BF16)] * 2,
        compiler_params=pltpu.CompilerParams(vmem_limit_bytes=VMEM_LIMIT),
        cost_estimate=pl.CostEstimate(
            flops=4 * count * size * size * size, bytes_accessed=4 * count * size * size, transcendentals=0
        ),
        name="order",
    )(columns, right)


def build_kernel(bits_ref, *refs):
    own_ref, (right_high, right_low, place_ref, high_ref, low_ref) = refs[:-5], refs[-5:]
    flat = lambda value: value.reshape(-1, value.shape[-1])
    left = halves(jnp.concatenate([flat(ref[:, 0, 0]) for ref in own_ref], axis=0))
    high, low = halves(product(left, (right_high[0], right_low[0])))
    size = high.shape[0]
    picks = lax.broadcasted_iota(jnp.int32, (size, size), 1) == place_ref[0]
    chosen = jnp.where(picks, 1.0, 0.0).astype(BF16)
    high_ref[0] = dot(chosen, high).astype(BF16)
    low_ref[0] = dot(chosen, low).astype(BF16)


def build(rows, starts, bits, rights, branch, wide, places):
    count, size, _ = places.shape
    width = rights[0].shape[1]
    shape = (count, size, wide)
    return pl.pallas_call(
        build_kernel,
        grid_spec=pltpu.PrefetchScalarGridSpec(
            num_scalar_prefetch=1,
            grid=(count,),
            in_specs=[
                pl.BlockSpec(
                    (value.shape[0], 1, 1) + value.shape[3:],
                    functools.partial(lambda start, t, bits: (0, t + start, bits[t], 0, 0), start),
                )
                for value, start in zip(rows, starts)
            ]
            + [pl.BlockSpec((1, width, wide), lambda t, bits: (t + branch, 0, 0))] * 2
            + [pl.BlockSpec((1, size, 1), lambda t, bits: (t, 0, 0))],
            out_specs=[pl.BlockSpec((1, size, wide), lambda t, bits: (t, 0, 0))] * 2,
        ),
        out_shape=[jax.ShapeDtypeStruct(shape, BF16)] * 2,
        compiler_params=pltpu.CompilerParams(vmem_limit_bytes=VMEM_LIMIT),
        cost_estimate=pl.CostEstimate(
            flops=10 * count * size * size * wide, bytes_accessed=8 * count * size * size, transcendentals=0
        ),
        name="build",
    )(bits, *rows, *rights, places)


def first_kernel(layout, x_ref, *refs):
    chunks, parts, inner = layout
    b0, b1, b2 = [(refs[0].at[t], refs[1].at[t]) for t in range(3)]
    outs, (high_ref, low_ref) = refs[2:-2], refs[-2:]
    size = b1[0].shape[0]
    half, quarter = size // 2, size // 4

    def lead(m4, carry):
        rows = jnp.concatenate(
            [
                x_ref[0, 0, pl.ds(pl.multiple_of(8 * m4, 8), 8), size * m : size * (m + 1)]
                for m in range(x_ref.shape[3] // size)
            ],
            axis=0,
        )
        index = lax.broadcasted_iota(jnp.int32, rows.shape, 0)
        eight, four = (index >> 3) & 1, (index >> 2) & 1
        rows = jnp.where(
            eight == four,
            rows,
            jnp.where(eight == 0, pltpu.roll(rows, rows.shape[0] - 4, 0), pltpu.roll(rows, 4, 0)),
        )
        value = product(halves(rows), (b0[0][...], b0[1][...]), ((1,), (1,)))
        value = value.reshape(half // 8, 2, 8, size)
        for m5 in range(2):
            part = value[:, m5].reshape(half, size)
            stacked = jnp.concatenate([part[:, :half], part[:, half:]], axis=0)
            result = product((b1[0][...], b1[1][...]), halves(stacked))
            high, low = halves(jnp.concatenate([result[:half], result[half:]], axis=1))
            place = pl.ds(pl.multiple_of((2 * m4 + m5) * quarter, quarter), quarter)
            for m13 in range(2):
                high_ref[m13, place, :] = high[m13 * quarter : (m13 + 1) * quarter]
                low_ref[m13, place, :] = low[m13 * quarter : (m13 + 1) * quarter]
        return carry

    lax.fori_loop(0, 2, lead, 0)

    def last(m13, carry):
        result = product((b2[0][...], b2[1][...]), (high_ref[m13], low_ref[m13]))
        for c, blocks in enumerate(chunks):
            for d in range(parts):
                for r, block in enumerate(blocks):
                    start = (block[0] * parts * inner + d * inner + block[1]) * (size // 16)
                    outs[c * parts + d][0, r, m13] = result[start : start + size // 16]
        return carry

    lax.fori_loop(0, 2, last, 0)


def first(stem, start, count, chunks, parts, inner, matrices):
    size = matrices[0].shape[1]
    trailing = stem.shape[3]
    lanes = size
    block = lambda c: (count, len(chunks[c]), 2, size // 16, lanes)
    whole = pl.BlockSpec((3, size, size), lambda k: (0, 0, 0))
    return pl.pallas_call(
        functools.partial(first_kernel, (chunks, parts, inner)),
        grid=(count,),
        in_specs=[pl.BlockSpec((1, 1, 16, trailing), lambda k: (0, k + start, 0, 0))] + [whole] * 2,
        out_specs=[
            pl.BlockSpec((1,) + block(c)[1:], lambda k: (k, 0, 0, 0, 0))
            for c in range(len(chunks))
            for _ in range(parts)
        ],
        out_shape=[
            jax.ShapeDtypeStruct(block(c), F32) for c in range(len(chunks)) for _ in range(parts)
        ],
        scratch_shapes=[pltpu.VMEM((2, size, size), BF16)] * 2,
        compiler_params=pltpu.CompilerParams(vmem_limit_bytes=VMEM_LIMIT),
        cost_estimate=pl.CostEstimate(
            flops=3 * 3 * 2 * count * 16 * trailing * size,
            bytes_accessed=8 * count * 16 * trailing,
            transcendentals=0,
        ),
        name="first",
    )(stem, *matrices)


def second_kernel(sources, pair_high, pair_low, b3h, b3l, *refs):
    inputs, (keep_ref, send_ref, high_ref, low_ref) = refs[:sources], refs[-4:]
    b4h, b5h, b4l, b5l = pair_high.at[0], pair_high.at[1], pair_low.at[0], pair_low.at[1]
    size = b5h.shape[0]
    half, quarter = size // 2, size // 4

    def head(m13, carry):
        rows = jnp.concatenate(
            [ref[k, 0, m13] for ref in inputs for k in range(ref.shape[0])], axis=0
        )
        rows = product(halves(rows), (b4h[...], b4l[...]), ((1,), (1,)))
        high, low = halves(product((b3h[0], b3l[0]), halves(rows)))
        high_ref[m13] = high
        low_ref[m13] = low
        return carry

    lax.fori_loop(0, 2, head, 0)
    states, _, depth, _ = keep_ref.shape[1:]

    def pair(lead, carry):
        place = pl.ds(pl.multiple_of(lead * quarter, quarter), quarter)
        stack = lambda ref: jnp.concatenate(
            [
                ref[m13, place, m14 * half : (m14 + 1) * half]
                for m13 in range(2)
                for m14 in range(2)
            ],
            axis=0,
        )
        result = product((b5h[...], b5l[...]), (stack(high_ref), stack(low_ref)))
        for q in range(states):
            keep_ref[0, q, lead] = result[q * depth : (q + 1) * depth]
            send_ref[0, q, lead] = result[(states + q) * depth : (states + q + 1) * depth]
        return carry

    lax.fori_loop(0, 4, pair, 0)


def second(inputs, matrices, devices_cuts):
    size = matrices[0].shape[1]
    rounds = inputs[0].shape[1]
    whole = lambda matrix: pl.BlockSpec(matrix.shape, lambda r: (0, 0, 0))
    shape = (rounds, devices_cuts // 2, 4, size // devices_cuts, size // 2)
    return pl.pallas_call(
        functools.partial(second_kernel, len(inputs)),
        grid=(rounds,),
        in_specs=[whole(matrix) for matrix in matrices]
        + [
            pl.BlockSpec((value.shape[0], 1) + value.shape[2:], lambda r: (0, r, 0, 0, 0))
            for value in inputs
        ],
        out_specs=[pl.BlockSpec((1,) + shape[1:], lambda r: (r, 0, 0, 0, 0))] * 2,
        out_shape=[jax.ShapeDtypeStruct(shape, F32)] * 2,
        scratch_shapes=[pltpu.VMEM((2, size, size), BF16)] * 2,
        compiler_params=pltpu.CompilerParams(vmem_limit_bytes=VMEM_LIMIT),
        cost_estimate=pl.CostEstimate(
            flops=3 * 2 * rounds * 4 * size * size * size,
            bytes_accessed=6 * rounds * size * size * 4,
            transcendentals=0,
        ),
        name="second",
    )(*matrices, *inputs)


def swap(value, axis, bit):
    count = lax.axis_size(axis)
    return lax.ppermute(value, axis, [(i, i ^ bit) for i in range(count)])


def scatter_sum(parts, at, descending):
    bits = parts[0].shape[1].bit_length() - 1
    arrays = [part.reshape(part.shape[:1] + (2,) * bits + part.shape[2:])[at] for part in parts]
    more, left = [], list(range(bits))
    for bit in range(bits) if descending else reversed(range(bits)):
        axis = left.index(bit)
        left.pop(axis)
        pick = lambda array, place: lax.index_in_dim(array, place, axis, keepdims=False)
        sent = functools.reduce(jnp.add, [pick(array, 1) for array in arrays])
        more.append(swap(sent, "cuts", 2 ** (bits - bit)))
        arrays = [pick(array, 0) for array in arrays] + more[-1:]
    return [(array, ()) for array in more]


def finish_kernel(inner, counts, *refs):
    refs, out_ref = list(refs[:-1]), refs[-1]
    states = out_ref.shape[0]
    for r in range(inner):
        terms = [refs.pop(0) for _ in range(counts[r])]
        total = functools.reduce(
            jnp.add, [ref[...].reshape(ref.shape[-2], ref.shape[-1]) for ref in terms]
        )
        rows, lanes = total.shape
        for row in range(rows):
            start = row % (rows // states) * lanes
            out_ref[row // (rows // states), r : r + 1, start : start + lanes] = total[row : row + 1]


def finish(terms, shape):
    flat = [term for block in terms for term in block]
    quarter = (shape[0] // 4,) + shape[1:]

    def spec(array, lead):
        front = array.ndim - 3 - len(lead)
        block = (1,) * (array.ndim - 2) + array.shape[-2:]
        return pl.BlockSpec(block, lambda a: tuple(lead) + (0,) * front + (a, 0, 0))

    return pl.pallas_call(
        functools.partial(finish_kernel, len(terms), [len(block) for block in terms]),
        grid=(4,),
        in_specs=[spec(array, lead) for array, lead in flat],
        out_specs=pl.BlockSpec(quarter, lambda a: (a, 0, 0)),
        out_shape=jax.ShapeDtypeStruct(shape, F32),
        compiler_params=pltpu.CompilerParams(vmem_limit_bytes=VMEM_LIMIT),
        name="finish",
    )(*[array for array, _ in flat])


def gather_rows(left, start, count, share):
    devices_mode, devices_cuts = lax.axis_size("mode"), lax.axis_size("cuts")
    own = left[start : start + count]
    piece = lax.dynamic_slice_in_dim(own, lax.axis_index("cuts") * share, share, 2)
    held = jnp.stack([swap(piece, "mode", d) for d in range(1, devices_mode)])
    near = [held] + [swap(held, "cuts", 2 * d) for d in range(1, devices_cuts // 2)]
    return near + [swap(value, "cuts", 1) for value in near]


def per_device(stem, left, right, slice_bits, leg_order):
    _, leading, _, trailing = stem.shape
    leg_count = leg_order.shape[1]
    size = 2**leg_count
    devices_mode, devices_cuts = lax.axis_size("mode"), lax.axis_size("cuts")
    mode, cut = lax.axis_index("mode"), lax.axis_index("cuts")
    parts = devices_mode // 2
    inner = 16 // devices_mode
    sixteenth = size // 16
    low = mode % parts
    n = jnp.arange(size, dtype=jnp.int32)

    depth = left.shape[2]
    share = depth // devices_cuts
    direct = direct_rows(depth, devices_cuts)
    if direct:
        early_rows = [left] + gather_rows(left, 0, 3, share)
        late_rows = [left] + gather_rows(left, 3, 3, share)
        early_rows[0] = late_rows[0] = left[None]
        starts = lambda first, offset: [first] + [offset] * (len(early_rows) - 1)
    else:
        early_rows, late_rows = ([lax.all_gather(left[s : s + 3], "mode")] for s in (0, 3))
        starts = lambda first, offset: [offset]

    def position(row):
        if not direct:
            return row
        far, near = (row // depth) ^ mode, (row % depth // share) ^ cut
        slot = (near % 2) * (devices_cuts // 2) + near // 2
        return jnp.where(
            far == 0,
            row % depth,
            depth + (slot * (devices_mode - 1) + far - 1) * share + row % share,
        )

    bit = lambda value, place: (value >> place) & 1
    columns_1 = bit(n, 1) * 256 + bit(n, 0) * 128 + (n >> 3 & 31) * 4 + bit(n, 2) * 2 + bit(n, 8)
    rows_1 = (n & 127) * 4 + bit(n, 7) * 2 + bit(n, 8)
    rows_2 = (((n // sixteenth) ^ (mode * inner)) * sixteenth) + n % sixteenth
    h = jnp.arange(size // 2, dtype=jnp.int32)
    local = h // sixteenth
    source = (local // leading) ^ low
    columns_3 = (
        (mode // parts) * (size // 2)
        + (source * leading + local % leading) * sixteenth
        + h % sixteenth
    )
    columns_5 = (n & 127) * 4 + (n >> 7)
    run = size // 4 // devices_cuts
    place = n // (size // devices_cuts)
    relative = (place % (devices_cuts // 2)) * 2 + place // (devices_cuts // 2)
    rest = n % (size // devices_cuts)
    rows_5 = (rest // run) * (size // 4) + (relative ^ cut) * run + rest % run
    columns = (n, columns_1, n, jnp.concatenate([columns_3, columns_3]), n, columns_5)
    rows = (n, rows_1, rows_2, n, n, rows_5)
    chosen = [leg_columns(leg_order[t], leg_count, columns[t]) for t in range(6)]
    rights = order(right, jnp.stack(chosen)[:, None, :])

    def matrices(branches, gathered, first, wide):
        places = jnp.stack([position(rows[t]) for t in branches])[:, :, None]
        bits = slice_bits[0, branches[0] : branches[-1] + 1]
        at = branches[0]
        return build(gathered, starts(at, at - first), bits, rights, at, wide, places)

    chunks, calls = plan(devices_mode)
    early = matrices((0, 1, 2), early_rows, 0, size)
    pieces = []
    for call in range(calls):
        per_call = leading // calls
        pieces.append(first(stem, call * per_call, per_call, chunks, parts, inner, early))
    arrived = [
        [
            pieces[call][c * parts + d]
            if d == 0
            else swap(pieces[call][c * parts + d], "mode", d)
            for d in range(parts)
            for call in range(calls)
        ]
        for c in range(len(chunks))
    ]
    late = [*matrices((4, 5), late_rows, 3, size), *matrices((3,), late_rows, 3, size // 2)]
    terms, far = {}, {}
    for c, blocks in enumerate(chunks):
        keep, send = second(arrived[c], late, devices_cuts)
        received = swap(send, "cuts", 1)
        for r, block in enumerate(blocks):
            more = scatter_sum((keep, received), r, block[1] % 2 == 0)
            terms[block] = [(keep, (r,)), (received, (r,))] + more
        if blocks[0][0] == 1:
            sums = [
                functools.reduce(jnp.add, [own(array, lead) for array, lead in terms[block]])
                for block in blocks
            ]
            arrival = swap(jnp.stack(sums), "mode", parts)
            far.update({block[1]: (arrival, (r,)) for r, block in enumerate(blocks)})
    summed = [terms[(0, r)] + [far[r]] for r in range(inner)]
    shape = (leading * devices_mode, inner, trailing // devices_cuts)
    return finish(summed, shape)


def own(array, lead):
    return array[tuple(lead) + (0,) * (array.ndim - 3 - len(lead))]


def direct_rows(depth, devices_cuts):
    return depth % (8 * devices_cuts) == 0


def plan(devices_mode):
    inner = 16 // devices_mode
    group = max(inner // 2, 1)
    chunks = tuple(
        tuple((m4, r) for r in range(start, start + group))
        for m4 in (1, 0)
        for start in range(0, inner, group)
    )
    return chunks, 2 if inner % 2 == 0 else 1


def solution(mesh):
    in_specs = (
        P("cuts", "mode", None, None),
        P(None, None, "mode", None),
        P(),
        P("cuts", None),
        P(),
    )
    out_specs = P(None, "mode", "cuts")

    return jax.shard_map(
        per_device, mesh=mesh, in_specs=in_specs, out_specs=out_specs, check_vma=False
    )
```
